32 devices in a mesh: section: 2 (over y), row: 4 (over x, core), col: 4 (over z).
Axes of the slice: x: 2, y: 2, z: 4, core: 2. Of those that a mesh axis runs over, the one named last changes fastest.
Arguments:
- inputs: float32 [3, 128, 16384], P(None, None, ('row', 'col')), may hold values from -512 to 512
- weights: float32 [2, 4, 4, 1024, 16384], P('section', None, 'col', None, 'row'), may hold values from -1 to 1
- norm_gain: float32 [2, 16384], P('section', ('row', 'col')), may hold values from 0.5 to 1.5
Outputs:
- section_outputs: float32 [2, 3, 128, 16384], P('section', None, None, ('row', 'col'))
The draws below stay inside these ranges and needn't reach their ends.
All inputs are finite; a program needn't handle non-finite values.
Results may differ from the reference program's by a relative error of at most 0.00036.
Values sent between devices are 32-bit elements; how exact they have to be, the bound alone decides.
A program may use at most 192 MiB of HBM per device.

```python
import math
import jax
import jax.numpy as jnp
from jax import lax

D = 16384
B = 128
M = 3
LAYERS = 2
ROW_BLOCKS = 4
COL_BLOCKS = 4
PIECE = 1024


offset_scale = 64.0


def shared_basis(key):
    raw_draw = jax.random.normal(jax.random.fold_in(key, 7103), (D, M * B), jnp.float32)
    basis_cols, upper_part = jnp.linalg.qr(raw_draw)
    return basis_cols


def draw_inputs(key, part):
    basis_cols = shared_basis(key)
    count = M * B
    mixing = jax.random.normal(jax.random.fold_in(key, 211), (count, count), jnp.float32) / math.sqrt(count)
    amplitude = jnp.ones((count, 1), jnp.float32)
    rough = jax.random.normal(jax.random.fold_in(key, 229), (count, D), jnp.float32)
    along = jnp.dot(mixing, basis_cols.T, precision=lax.Precision.HIGHEST)
    large = offset_scale * math.sqrt(D) * amplitude * along
    values = jnp.clip(large + rough, -512.0, 512.0)
    return values.reshape(M, B, D)


def draw_weights(key, part):
    basis_cols = shared_basis(key)
    matrices = []
    for level in range(LAYERS):
        layer_key = jax.random.fold_in(key, 401 + level)
        dense = jnp.clip(jax.random.normal(layer_key, (D, D), jnp.float32), -6.0, 6.0) / math.sqrt(D)
        inside = jnp.dot(basis_cols.T, dense, precision=lax.Precision.HIGHEST)
        matrix = dense - (1.0 - 1.0 / offset_scale) * jnp.dot(basis_cols, inside, precision=lax.Precision.HIGHEST)
        matrices.append(matrix.reshape(ROW_BLOCKS, COL_BLOCKS, PIECE, D))
    return jnp.stack(matrices)


def setup_inputs(seed: int = 0) -> dict:
    key_of = jax.random.split(jax.random.key(seed), 4)
    return {
        "inputs": draw_inputs(jax.random.fold_in(key_of[3], 71), 0),
        "weights": draw_weights(jax.random.fold_in(key_of[3], 71), 0),
        "norm_gain": jnp.clip(1.0 + 0.1 * jax.random.normal(key_of[2], (LAYERS, D), jnp.float32), 0.5, 1.5),
    }


def split_two(values):
    first = lax.optimization_barrier(values.astype(jnp.bfloat16))
    second = lax.optimization_barrier((values - first.astype(jnp.float32)).astype(jnp.bfloat16))
    return (first, second)

def widen(values):
    return values.astype(jnp.float32)

def layer(activations, matrix, gain):
    first, second = split_two(activations)
    sum_two = widen(first) + widen(second)
    sum_one = widen(first)
    width = matrix.shape[1]
    block_cols = width // 8

    def column_block(index):
        cols = lax.dynamic_slice_in_dim(matrix, (index * block_cols).astype(jnp.int32), block_cols, 1)
        wfirst, wsecond = split_two(cols)
        total = jnp.dot(sum_two.astype(jnp.float32), widen(wfirst).astype(jnp.float32), precision=lax.Precision.HIGHEST, preferred_element_type=jnp.float32)
        total = total + jnp.dot(sum_one.astype(jnp.float32), widen(wsecond).astype(jnp.float32), precision=lax.Precision.HIGHEST, preferred_element_type=jnp.float32)
        return total
    blocks = lax.map(column_block, jnp.arange(8, dtype=jnp.int32))
    summed = jnp.transpose(blocks, (1, 0, 2)).reshape(activations.shape[0], width)
    active = jax.nn.gelu(summed, approximate=True)
    squares = lax.optimization_barrier(jnp.sum(active * active, axis=1))
    scale = lax.rsqrt(squares / width + 1e-06)
    return active * scale[:, None] * gain[None, :]

def reference(inputs, weights, norm_gain):
    current = inputs.reshape(M * B, D)
    results = []
    for level in range(LAYERS):
        matrix = weights[level].reshape(D, D)
        branch = layer(current, matrix, norm_gain[level])
        results.append(branch.reshape(M, B, D))
        current = current + branch
    return jnp.stack(results)
```

```python
import functools

import jax
import jax.numpy as jnp
from jax import lax
from jax.experimental import pallas as pl
from jax.experimental.pallas import tpu as pltpu
from jax.sharding import PartitionSpec as P

MESH = pl.DeviceIdType.MESH
SPAN = 16
RING = 3
KEEP = 4
PARTS = 2


def slices(values):
    first = values.astype(jnp.bfloat16)
    second = (values - first.astype(jnp.float32)).astype(jnp.bfloat16)
    return first, second


def sending_order(col_count):
    table = []
    for here in range(col_count):
        keys = []
        for there in range(col_count):
            if there > here:
                keys.append((col_count - 1 - there + here, there))
            elif there < here:
                keys.append((there + col_count - 1 - here, there))
        table.append([there for _, there in sorted(keys)] + [here])
    return table


def kernel(
    sections, row_count, col_count,
    x_ref, w_ref, gain_ref, out_ref,
    gathered, branch, lhs, part, landed, scaled, squares, factor, factor_in, tiles,
    col_out, col_in, row_out, row_in,
    tile_sem, gx_send, gx_recv, gy_send, gy_recv, rs_send, rs_recv,
    col_send, col_recv, row_send, row_recv, next_send, next_recv, fac_send, fac_recv,
):
    groups, rows, pieces = x_ref.shape
    width = tiles.shape[2]
    per_chunk = pieces // width
    steps = per_chunk * col_count
    kept = steps // KEEP
    total_features = pieces * row_count * col_count
    section = lax.axis_index("section")
    row = lax.axis_index("row")
    col = lax.axis_index("col")
    cores = 2 if row_count % 2 == 0 else 1
    chips = row_count // cores
    core = lax.rem(row, cores)
    chip = row // cores
    edge = (col == 0) | (col == col_count - 1)
    inner = (col > 0) & (col < col_count - 1)
    first_section = section == 0
    table = sending_order(col_count)

    def passing(k):
        found = jnp.int32(0)
        for here in range(col_count):
            for place in range(col_count):
                found = jnp.where((col == here) & (k == place), table[here][place], found)
        return found

    def around(position, step, count):
        return lax.rem(position + step, count)

    def chip_row(step, which):
        return around(chip, step, chips) * cores + which

    def remote(src, dst, send, recv, device):
        return pltpu.make_async_remote_copy(
            src_ref=src, dst_ref=dst, send_sem=send, recv_sem=recv,
            device_id=device, device_id_type=MESH,
        )

    def slot_of(m, q):
        stream = m * (steps - kept) + q - q // KEEP - 1
        return jnp.where(lax.rem(q, KEEP) == 0, RING + q // KEEP, lax.rem(jnp.maximum(stream, 0), RING))

    def fetch(m, q):
        start = passing(q // per_chunk) * pieces + lax.rem(q, per_chunk) * width
        slot = slot_of(m, q)
        return pltpu.make_async_copy(
            w_ref.at[:, pl.ds(pl.multiple_of(start, width), width)],
            tiles.at[slot], tile_sem.at[slot],
        )

    def fetched(m, q):
        return (m == 0) | (lax.rem(q, KEEP) != 0)

    for q in range(RING):
        fetch(0, q).start()

    barrier = pltpu.get_barrier_semaphore()
    for step in range(1, row_count):
        pl.semaphore_signal(barrier, inc=1, device_id={"row": around(row, step, row_count)}, device_id_type=MESH)
    for step in range(1, col_count):
        pl.semaphore_signal(barrier, inc=1, device_id={"col": around(col, step, col_count)}, device_id_type=MESH)

    @pl.when(section > 0)
    def _():
        pl.semaphore_signal(barrier, inc=1, device_id={"section": section - 1}, device_id_type=MESH)

    @pl.when(section < sections - 1)
    def _():
        pl.semaphore_signal(barrier, inc=1, device_id={"section": section + 1}, device_id_type=MESH)

    before = (section + sections - 1) // sections
    after = (2 * (sections - 1) - section) // sections
    pl.semaphore_wait(barrier, row_count + col_count - 2 + before + after)

    def gather_send(buffer, send, recv, m, target):
        return remote(buffer.at[m, row], buffer.at[m, row], send.at[m, target], recv.at[m, row], {"row": target})

    def gather_start(buffer, send, recv, m):
        for step in range(1, chips):
            gather_send(buffer, send, recv, m, chip_row(step, core)).start()
        if cores == 2:
            gather_send(buffer, send, recv, m, chip * cores + 1 - core).start()

    def gather_forward(buffer, send, recv, m, step):
        held = chip_row(step, core)
        slot = chip_row(step, 1 - core)
        return remote(
            buffer.at[m, held], buffer.at[m, held], send.at[m, slot],
            recv.at[m, held], {"row": chip * cores + 1 - core},
        )

    def gather_landed(buffer, send, recv, m, source):
        target = around(row, 1, row_count)
        remote(buffer.at[m, source], buffer.at[m, source], send.at[m, source],
               recv.at[m, source], {"row": target}).wait_recv()

    def gather_relay(buffer, send, recv, m):
        for step in range(1, chips):
            gather_landed(buffer, send, recv, m, chip_row(step, core))
            if cores == 2:
                gather_forward(buffer, send, recv, m, step).start()

    def gather_rest(buffer, send, recv, m):
        if cores == 2:
            for step in range(chips):
                gather_landed(buffer, send, recv, m, chip_row(step, 1 - core))

    def gather_drain(buffer, send, recv, m):
        for step in range(1, chips):
            gather_send(buffer, send, recv, m, chip_row(step, core)).wait_send()
            if cores == 2:
                gather_forward(buffer, send, recv, m, step).wait_send()
        if cores == 2:
            gather_send(buffer, send, recv, m, chip * cores + 1 - core).wait_send()

    gx = (gathered, gx_send, gx_recv)
    gy = (branch, gy_send, gy_recv)

    def x_start(m):
        gathered[m, row] = x_ref[m]
        gather_start(*gx, m)

    def hand(m, target):
        return remote(scaled.at[m], branch.at[m, row], next_send.at[m], next_recv.at[m], {"section": target})

    def hand_factor(m, target):
        return remote(factor.at[m], factor_in.at[m], fac_send.at[m], fac_recv.at[m], {"section": target})

    def unit(m, there):
        upward = (there > col).astype(jnp.int32)
        slot = there + upward
        return remote(part.at[m, there], landed.at[m, slot], rs_send.at[m, there],
                      rs_recv.at[m, slot], {"col": col + 2 * upward - 1})

    def take(m, slot, there):
        remote(part.at[m, there], landed.at[m, slot], rs_send.at[m, there],
               rs_recv.at[m, slot], {"col": around(col, 1, col_count)}).wait_recv()

        def grow(g, carry):
            span = pl.ds(pl.multiple_of(g * SPAN, SPAN), SPAN)
            part[m, there, span, :] += landed[m, slot, span, :]
            return carry
        lax.fori_loop(0, rows // SPAN, grow, 0)

    def forward(m, k):
        there = passing(k)
        take(m, there + (there > col).astype(jnp.int32), there)
        unit(m, there).start()

    def issue(m, i):
        @pl.when(i > 0)
        def _():
            unit(m, passing(i - 1)).wait_send()

        @pl.when((i == 0) & (m > 0))
        def _():
            unit(m - 1, passing(col_count - 2)).wait_send()
        unit(m, passing(i)).start()

    def share_start(m, outgoing, incoming, send, recv, axis, position, count):
        for step in range(1, count):
            target = around(position, step, count)
            remote(outgoing.at[m], incoming.at[m, position], send.at[m, target],
                   recv.at[m, position], {axis: target}).start()

    def share_total(m, outgoing, incoming, send, recv, axis, position, count):
        total = outgoing[m]
        for step in range(1, count):
            source = around(position, step, count)
            remote(outgoing.at[m], incoming.at[m, source], send.at[m, source],
                   recv.at[m, source], {axis: source}).wait_recv()
            total = total + incoming[m, source]
        for step in range(1, count):
            target = around(position, step, count)
            remote(outgoing.at[m], incoming.at[m, position], send.at[m, target],
                   recv.at[m, position], {axis: target}).wait_send()
        return total

    by_row = (row_out, row_in, row_send, row_recv, "row", row, row_count)
    by_col = (col_out, col_in, col_send, col_recv, "col", col, col_count)

    def activate(m):
        @pl.when(col > 0)
        def _():
            take(m, col + 1, col)

        @pl.when(col < col_count - 1)
        def _():
            take(m, col, col)

        def spans(g, carry):
            span = pl.ds(pl.multiple_of(g * SPAN, SPAN), SPAN)
            y = jax.nn.gelu(part[m, col, span, :], approximate=True)
            scaled[m, span, :] = y * gain_ref[...]
            squares[span, :] = jnp.broadcast_to(jnp.sum(y * y, axis=1, keepdims=True), (SPAN, 128))
            return carry
        lax.fori_loop(0, rows // SPAN, spans, 0)

        @pl.when(section < sections - 1)
        def _():
            hand(m, section + 1).start()
        row_out[m] = squares[...].T[:8]
        share_start(m, *by_row)
        col_out[m] = share_total(m, *by_row)
        share_start(m, *by_col)

    def normalize(m):
        total = share_total(m, *by_col)
        scale = lax.rsqrt(total[:1] / total_features + 1e-06)
        squares[...] = jnp.broadcast_to(scale, (128, 128)).T
        factor[m] = squares[:rows]

        @pl.when(section < sections - 1)
        def _():
            hand_factor(m, section + 1).start()

        def spans(g, carry):
            span = pl.ds(pl.multiple_of(g * SPAN, SPAN), SPAN)
            out_ref[m, span, :] = scaled[m, span, :] * factor[m, span, :1]
            return carry
        lax.fori_loop(0, rows // SPAN, spans, 0)

    def prepare(m, added):
        def body(r, carry):
            lanes = pl.ds(pl.multiple_of(r * pieces, pieces), pieces)
            for start in range(0, rows, SPAN):
                values = gathered[m, r, start:start + SPAN]
                if added:
                    values = values + branch[m, r, start:start + SPAN] * factor_in[m, start:start + SPAN, :1]
                first, second = slices(values)
                lhs[start:start + SPAN, lanes] = first
                lhs[rows + start:rows + start + SPAN, lanes] = second
            return carry
        lax.fori_loop(0, row_count, body, 0)

    def acquire(m):
        @pl.when(first_section)
        def _():
            @pl.when(m == 0)
            def _():
                gather_relay(*gx, m)
            gather_rest(*gx, m)

            @pl.when(m + 1 < groups)
            def _():
                x_start(m + 1)
            prepare(m, False)

        @pl.when(section > 0)
        def _():
            @pl.when(m == 0)
            def _():
                def early(n, carry):
                    gather_relay(*gx, n)
                    gather_rest(*gx, n)
                    return carry
                lax.fori_loop(0, groups, early, 0)
                hand(m, section - 1).wait_recv()
                gather_start(*gy, m)
            gather_relay(*gy, m)
            gather_rest(*gy, m)
            hand_factor(m, section - 1).wait_recv()
            prepare(m, True)

    def multiply(m, i):
        there = passing(i)

        def tile_body(j, carry):
            q = i * per_chunk + j
            ahead = m * steps + q + RING
            ahead_m = ahead // steps
            ahead_q = lax.rem(ahead, steps)

            @pl.when((ahead < groups * steps) & fetched(ahead_m, ahead_q))
            def _():
                fetch(ahead_m, ahead_q).start()

            @pl.when(fetched(m, q))
            def _():
                fetch(m, q).wait()
            first, second = slices(tiles[slot_of(m, q)])
            both = jnp.dot(lhs[...], first, preferred_element_type=jnp.float32)
            low = jnp.dot(lhs[:rows], second, preferred_element_type=jnp.float32)
            part[m, there, :, pl.ds(pl.multiple_of(j * width, width), width)] = both[:rows] + (both[rows:] + low)
            return carry
        lax.fori_loop(0, per_chunk, tile_body, 0)

    @pl.when(first_section)
    def _():
        x_start(0)

    @pl.when(section > 0)
    def _():
        def begin(m, carry):
            x_start(m)
            return carry
        lax.fori_loop(0, groups, begin, 0)

    def group_body(m, carry):
        last = m - 1

        @pl.when(m < groups)
        def _():
            acquire(m)

        def chunk_body(i, carry):
            @pl.when(m < groups)
            def _():
                multiply(m, i)

            @pl.when((i == 0) & (m > 0) & inner)
            def _():
                def rest(k, carry):
                    forward(last, k)
                    return carry
                lax.fori_loop(2, col_count - 1, rest, 0)

            turn = jnp.where(m == 1, 0, 1)

            @pl.when((i == turn) & (m > 0))
            def _():
                activate(last)

            @pl.when((i < col_count - 1) & (m < groups) & edge)
            def _():
                issue(m, i)

            @pl.when((i >= col_count - 2) & (m < groups) & inner)
            def _():
                forward(m, i - (col_count - 2))

            @pl.when((i == turn + 1) & (m > 0))
            def _():
                normalize(last)

            @pl.when((i == col_count - 2) & (m + 1 < groups))
            def _():
                @pl.when(first_section)
                def _():
                    gather_relay(*gx, m + 1)

                @pl.when(section > 0)
                def _():
                    hand(m + 1, section - 1).wait_recv()
                    gather_start(*gy, m + 1)
            return carry
        lax.fori_loop(0, col_count, chunk_body, 0)
        return carry
    lax.fori_loop(0, groups + 1, group_body, 0)

    @pl.when(edge)
    def _():
        unit(groups - 1, passing(col_count - 2)).wait_send()

    def drain(m, carry):
        gather_drain(*gx, m)

        @pl.when(section > 0)
        def _():
            gather_drain(*gy, m)

        @pl.when(section < sections - 1)
        def _():
            hand(m, section + 1).wait_send()
            hand_factor(m, section + 1).wait_send()

        @pl.when(inner)
        def _():
            def sent(k, carry):
                unit(m, passing(k)).wait_send()
                return carry
            lax.fori_loop(0, col_count - 1, sent, 0)
        return carry
    lax.fori_loop(0, groups, drain, 0)


def solution(mesh):
    sections, row_count, col_count = (mesh.shape[name] for name in ("section", "row", "col"))

    def shards(inputs, weights, norm_gain):
        micro, batch, pieces = inputs.shape
        groups, rows = micro * PARTS, batch // PARTS
        depth = row_count * pieces
        out_cols = weights.shape[4]
        width = min(256, pieces)
        kept = (out_cols // width) // KEEP
        f32 = jnp.float32
        dma = pltpu.SemaphoreType.DMA
        result = pl.pallas_call(
            functools.partial(kernel, sections, row_count, col_count),
            out_shape=jax.ShapeDtypeStruct((groups, rows, pieces), f32),
            in_specs=[
                pl.BlockSpec(memory_space=pltpu.VMEM),
                pl.BlockSpec(memory_space=pltpu.HBM),
                pl.BlockSpec(memory_space=pltpu.VMEM),
            ],
            out_specs=pl.BlockSpec(memory_space=pltpu.VMEM),
            scratch_shapes=[
                pltpu.VMEM((groups, row_count, rows, pieces), f32),
                pltpu.VMEM((groups, row_count, rows, pieces), f32),
                pltpu.VMEM((2 * rows, depth), jnp.bfloat16),
                pltpu.VMEM((groups, col_count, rows, pieces), f32),
                pltpu.VMEM((groups, col_count + 1, rows, pieces), f32),
                pltpu.VMEM((groups, rows, pieces), f32),
                pltpu.VMEM((128, 128), f32),
                pltpu.VMEM((groups, rows, 128), f32),
                pltpu.VMEM((groups, rows, 128), f32),
                pltpu.VMEM((RING + kept, depth, width), f32),
                pltpu.VMEM((groups, 8, 128), f32),
                pltpu.VMEM((groups, col_count, 8, 128), f32),
                pltpu.VMEM((groups, 8, 128), f32),
                pltpu.VMEM((groups, row_count, 8, 128), f32),
                dma((RING + kept,)),
                dma((groups, row_count)),
                dma((groups, row_count)),
                dma((groups, row_count)),
                dma((groups, row_count)),
                dma((groups, col_count)),
                dma((groups, col_count + 1)),
                dma((groups, col_count)),
                dma((groups, col_count)),
                dma((groups, row_count)),
                dma((groups, row_count)),
                dma((groups,)),
                dma((groups,)),
                dma((groups,)),
                dma((groups,)),
            ],
            compiler_params=pltpu.CompilerParams(
                collective_id=0, has_side_effects=True, vmem_limit_bytes=67043328
            ),
        )(inputs.reshape(groups, rows, pieces), weights.reshape(depth, out_cols), norm_gain)
        return result.reshape(1, micro, batch, pieces)

    placed = (
        P(None, None, ("row", "col")),
        P("section", None, "col", None, "row"),
        P("section", ("row", "col")),
    )
    return jax.shard_map(
        shards,
        mesh=mesh,
        in_specs=placed,
        out_specs=P("section", None, None, ("row", "col")),
        check_vma=False,
    )
```

```python
import functools

import jax
import jax.numpy as jnp
from jax import lax
from jax.experimental import pallas as pl
from jax.experimental.pallas import tpu as pltpu
from jax.sharding import PartitionSpec as P

MESH = pl.DeviceIdType.MESH
SPAN = 16
RING = 3
KEEP = 4
PARTS = 2
LAG = 2
ACT = 2
PASS = 3
NORM = 2


def slices(values):
    first = values.astype(jnp.bfloat16)
    second = (values - first.astype(jnp.float32)).astype(jnp.bfloat16)
    return first, second


def sending_order(col_count):
    table = []
    for here in range(col_count):
        keys = []
        for there in range(col_count):
            if there > here:
                keys.append((col_count - 1 - there + here, there))
            elif there < here:
                keys.append((there + col_count - 1 - here, there))
        table.append([there for _, there in sorted(keys)] + [here])
    return table


def kernel(
    sections, row_count, col_count,
    x_ref, w_ref, gain_ref, out_ref,
    gathered, branch, lhs, part, landed, scaled, squares, factor, factor_in, tiles,
    col_out, col_in, row_out, row_in,
    tile_sem, gx_send, gx_recv, gy_send, gy_recv, rs_send, rs_recv,
    col_send, col_recv, row_send, row_recv, next_send, next_recv, fac_send, fac_recv,
):
    groups, rows, pieces = x_ref.shape
    width = tiles.shape[2]
    per_chunk = pieces // width
    steps = per_chunk * col_count
    kept = steps // KEEP
    total_features = pieces * row_count * col_count
    section = lax.axis_index("section")
    row = lax.axis_index("row")
    col = lax.axis_index("col")
    cores = 2 if row_count % 2 == 0 else 1
    chips = row_count // cores
    core = lax.rem(row, cores)
    chip = row // cores
    edge = (col == 0) | (col == col_count - 1)
    inner = (col > 0) & (col < col_count - 1)
    first_section = section == 0
    table = sending_order(col_count)

    places = []
    for place in range(col_count):
        found = jnp.int32(table[0][place])
        for here in range(1, col_count):
            found = jnp.where(col == here, table[here][place], found)
        places.append(found)

    def passing(k):
        found = places[0]
        for place in range(1, col_count):
            found = jnp.where(k == place, places[place], found)
        return found

    def around(position, step, count):
        return lax.rem(position + step, count)

    def chip_row(step, which):
        return around(chip, step, chips) * cores + which

    def remote(src, dst, send, recv, device):
        return pltpu.make_async_remote_copy(
            src_ref=src, dst_ref=dst, send_sem=send, recv_sem=recv,
            device_id=device, device_id_type=MESH,
        )

    def slot_of(m, q):
        stream = m * (steps - kept) + q - q // KEEP - 1
        return jnp.where(lax.rem(q, KEEP) == 0, RING + q // KEEP, lax.rem(jnp.maximum(stream, 0), RING))

    def fetch(m, q):
        start = passing(q // per_chunk) * pieces + lax.rem(q, per_chunk) * width
        slot = slot_of(m, q)
        return pltpu.make_async_copy(
            w_ref.at[:, pl.ds(pl.multiple_of(start, width), width)],
            tiles.at[slot], tile_sem.at[slot],
        )

    def fetched(m, q):
        return (m == 0) | (lax.rem(q, KEEP) != 0)

    for q in range(RING):
        fetch(0, q).start()

    barrier = pltpu.get_barrier_semaphore()
    for step in range(1, row_count):
        pl.semaphore_signal(barrier, inc=1, device_id={"row": around(row, step, row_count)}, device_id_type=MESH)
    for step in range(1, col_count):
        pl.semaphore_signal(barrier, inc=1, device_id={"col": around(col, step, col_count)}, device_id_type=MESH)

    @pl.when(section > 0)
    def _():
        pl.semaphore_signal(barrier, inc=1, device_id={"section": section - 1}, device_id_type=MESH)

    @pl.when(section < sections - 1)
    def _():
        pl.semaphore_signal(barrier, inc=1, device_id={"section": section + 1}, device_id_type=MESH)

    before = (section + sections - 1) // sections
    after = (2 * (sections - 1) - section) // sections
    pl.semaphore_wait(barrier, row_count + col_count - 2 + before + after)

    def gather_send(buffer, send, recv, m, target):
        return remote(buffer.at[m, row], buffer.at[m, row], send.at[m, target], recv.at[m, row], {"row": target})

    def gather_start(buffer, send, recv, m):
        for step in range(1, chips):
            gather_send(buffer, send, recv, m, chip_row(step, core)).start()
        if cores == 2:
            gather_send(buffer, send, recv, m, chip * cores + 1 - core).start()

    def gather_forward(buffer, send, recv, m, step):
        held = chip_row(step, core)
        slot = chip_row(step, 1 - core)
        return remote(
            buffer.at[m, held], buffer.at[m, held], send.at[m, slot],
            recv.at[m, held], {"row": chip * cores + 1 - core},
        )

    def gather_landed(buffer, send, recv, m, source):
        target = around(row, 1, row_count)
        remote(buffer.at[m, source], buffer.at[m, source], send.at[m, source],
               recv.at[m, source], {"row": target}).wait_recv()

    def gather_relay(buffer, send, recv, m):
        for step in range(1, chips):
            gather_landed(buffer, send, recv, m, chip_row(step, core))
            if cores == 2:
                gather_forward(buffer, send, recv, m, step).start()

    def gather_rest(buffer, send, recv, m):
        if cores == 2:
            for step in range(chips):
                gather_landed(buffer, send, recv, m, chip_row(step, 1 - core))

    def gather_drain(buffer, send, recv, m):
        for step in range(1, chips):
            gather_send(buffer, send, recv, m, chip_row(step, core)).wait_send()
            if cores == 2:
                gather_forward(buffer, send, recv, m, step).wait_send()
        if cores == 2:
            gather_send(buffer, send, recv, m, chip * cores + 1 - core).wait_send()

    gx = (gathered, gx_send, gx_recv)
    gy = (branch, gy_send, gy_recv)

    def x_start(m):
        gathered[m, row] = x_ref[m]
        gather_start(*gx, m)

    def hand(m, target):
        return remote(scaled.at[m], branch.at[m, row], next_send.at[m], next_recv.at[m], {"section": target})

    def hand_factor(m, target):
        return remote(factor.at[m], factor_in.at[m], fac_send.at[m], fac_recv.at[m], {"section": target})

    def unit(m, there):
        upward = (there > col).astype(jnp.int32)
        slot = there + upward
        return remote(part.at[m, there], landed.at[m, slot], rs_send.at[m, there],
                      rs_recv.at[m, slot], {"col": col + 2 * upward - 1})

    def take(m, slot, there):
        remote(part.at[m, there], landed.at[m, slot], rs_send.at[m, there],
               rs_recv.at[m, slot], {"col": around(col, 1, col_count)}).wait_recv()

        def grow(g, carry):
            span = pl.ds(pl.multiple_of(g * SPAN, SPAN), SPAN)
            part[m, there, span, :] += landed[m, slot, span, :]
            return carry
        lax.fori_loop(0, rows // SPAN, grow, 0)

    def forward(m, k):
        there = passing(k)
        take(m, there + (there > col).astype(jnp.int32), there)
        unit(m, there).start()

    def issue(m, i):
        @pl.when(i >= LAG)
        def _():
            unit(m, passing(i - LAG)).wait_send()

        @pl.when((i < LAG) & (m > 0))
        def _():
            unit(m - 1, passing(col_count - 1 + i - LAG)).wait_send()
        unit(m, passing(i)).start()

    def share_start(m, outgoing, incoming, send, recv, axis, position, count):
        for step in range(1, count):
            target = around(position, step, count)
            remote(outgoing.at[m], incoming.at[m, position], send.at[m, target],
                   recv.at[m, position], {axis: target}).start()

    def share_total(m, outgoing, incoming, send, recv, axis, position, count):
        total = outgoing[m]
        for step in range(1, count):
            source = around(position, step, count)
            remote(outgoing.at[m], incoming.at[m, source], send.at[m, source],
                   recv.at[m, source], {axis: source}).wait_recv()
            total = total + incoming[m, source]
        for step in range(1, count):
            target = around(position, step, count)
            remote(outgoing.at[m], incoming.at[m, position], send.at[m, target],
                   recv.at[m, position], {axis: target}).wait_send()
        return total

    by_row = (row_out, row_in, row_send, row_recv, "row", row, row_count)
    by_col = (col_out, col_in, col_send, col_recv, "col", col, col_count)

    def activate(m):
        @pl.when(col > 0)
        def _():
            take(m, col + 1, col)

        @pl.when(col < col_count - 1)
        def _():
            take(m, col, col)

        def spans(g, carry):
            span = pl.ds(pl.multiple_of(g * SPAN, SPAN), SPAN)
            y = jax.nn.gelu(part[m, col, span, :], approximate=True)
            scaled[m, span, :] = y * gain_ref[...]
            squares[span, :] = jnp.broadcast_to(jnp.sum(y * y, axis=1, keepdims=True), (SPAN, 128))
            return carry
        lax.fori_loop(0, rows // SPAN, spans, 0)

        @pl.when(section < sections - 1)
        def _():
            hand(m, section + 1).start()
        row_out[m] = squares[...].T[:8]
        share_start(m, *by_row)

    def pass_on(m):
        col_out[m] = share_total(m, *by_row)
        share_start(m, *by_col)

    def normalize(m):
        total = share_total(m, *by_col)
        scale = lax.rsqrt(total[:1] / total_features + 1e-06)
        squares[...] = jnp.broadcast_to(scale, (128, 128)).T
        factor[m] = squares[:rows]

        @pl.when(section < sections - 1)
        def _():
            hand_factor(m, section + 1).start()

        def spans(g, carry):
            span = pl.ds(pl.multiple_of(g * SPAN, SPAN), SPAN)
            out_ref[m, span, :] = scaled[m, span, :] * factor[m, span, :1]
            return carry
        lax.fori_loop(0, rows // SPAN, spans, 0)

    def prepare(m, added):
        def body(r, carry):
            lanes = pl.ds(pl.multiple_of(r * pieces, pieces), pieces)
            for start in range(0, rows, SPAN):
                values = gathered[m, r, start:start + SPAN]
                if added:
                    values = values + branch[m, r, start:start + SPAN] * factor_in[m, start:start + SPAN, :1]
                first, second = slices(values)
                lhs[start:start + SPAN, lanes] = first
                lhs[rows + start:rows + start + SPAN, lanes] = second
            return carry
        lax.fori_loop(0, row_count, body, 0)

    def acquire(m):
        @pl.when(first_section)
        def _():
            @pl.when(m == 0)
            def _():
                gather_relay(*gx, m)
            gather_rest(*gx, m)

            @pl.when(m + 1 < groups)
            def _():
                x_start(m + 1)
            prepare(m, False)

        @pl.when(section > 0)
        def _():
            @pl.when(m == 0)
            def _():
                def early(n, carry):
                    gather_relay(*gx, n)
                    gather_rest(*gx, n)
                    return carry
                lax.fori_loop(0, groups, early, 0)
                hand(m, section - 1).wait_recv()
                gather_start(*gy, m)
            gather_relay(*gy, m)
            gather_rest(*gy, m)
            hand_factor(m, section - 1).wait_recv()
            prepare(m, True)

    def multiply(m, i):
        there = passing(i)

        def tile_body(j, carry):
            q = i * per_chunk + j
            ahead = m * steps + q + RING
            ahead_m = ahead // steps
            ahead_q = lax.rem(ahead, steps)

            @pl.when((ahead < groups * steps) & fetched(ahead_m, ahead_q))
            def _():
                fetch(ahead_m, ahead_q).start()

            @pl.when(fetched(m, q))
            def _():
                fetch(m, q).wait()
            first, second = slices(tiles[slot_of(m, q)])
            both = jnp.dot(lhs[...], first, preferred_element_type=jnp.float32)
            low = jnp.dot(lhs[:rows], second, preferred_element_type=jnp.float32)
            part[m, there, :, pl.ds(pl.multiple_of(j * width, width), width)] = both[:rows] + (both[rows:] + low)
            return carry
        lax.fori_loop(0, per_chunk, tile_body, 0)

    @pl.when(first_section)
    def _():
        x_start(0)

    @pl.when(section > 0)
    def _():
        def begin(m, carry):
            x_start(m)
            return carry
        lax.fori_loop(0, groups, begin, 0)

    def group_body(m, carry):
        last = m - 1

        @pl.when(m < groups)
        def _():
            acquire(m)

        def chunk_body(i, carry):
            @pl.when(m < groups)
            def _():
                multiply(m, i)

            @pl.when((i < col_count - 1) & (m < groups) & edge)
            def _():
                issue(m, i)

            @pl.when((i == 0) & (m > 0) & inner)
            def _():
                def rest(k, carry):
                    forward(last, k)
                    return carry
                lax.fori_loop(2, col_count - 1, rest, 0)

            @pl.when((i >= col_count - 2) & (m < groups) & inner)
            def _():
                forward(m, i - (col_count - 2))

            soon = (m == 1) | (m == groups)

            @pl.when((i == jnp.where(soon, 0, ACT)) & (m > 0))
            def _():
                activate(last)

            @pl.when((i == jnp.where(soon, 0, PASS)) & (m > 0))
            def _():
                pass_on(last)

            @pl.when((i == 0) & (m > 2))
            def _():
                normalize(m - 2)

            @pl.when((i == NORM) & soon)
            def _():
                normalize(last)

            @pl.when((i == col_count - 2) & (m + 1 < groups))
            def _():
                @pl.when(first_section)
                def _():
                    gather_relay(*gx, m + 1)

                @pl.when(section > 0)
                def _():
                    hand(m + 1, section - 1).wait_recv()
                    gather_start(*gy, m + 1)
            return carry
        lax.fori_loop(0, col_count, chunk_body, 0)
        return carry
    lax.fori_loop(0, groups + 1, group_body, 0)

    @pl.when(edge)
    def _():
        for i in range(LAG):
            unit(groups - 1, passing(col_count - 2 - i)).wait_send()

    def drain(m, carry):
        gather_drain(*gx, m)

        @pl.when(section > 0)
        def _():
            gather_drain(*gy, m)

        @pl.when(section < sections - 1)
        def _():
            hand(m, section + 1).wait_send()
            hand_factor(m, section + 1).wait_send()

        @pl.when(inner)
        def _():
            def sent(k, carry):
                unit(m, passing(k)).wait_send()
                return carry
            lax.fori_loop(0, col_count - 1, sent, 0)
        return carry
    lax.fori_loop(0, groups, drain, 0)


def solution(mesh):
    sections, row_count, col_count = (mesh.shape[name] for name in ("section", "row", "col"))

    def shards(inputs, weights, norm_gain):
        micro, batch, pieces = inputs.shape
        groups, rows = micro * PARTS, batch // PARTS
        depth = row_count * pieces
        out_cols = weights.shape[4]
        width = min(256, pieces)
        kept = (out_cols // width) // KEEP
        f32 = jnp.float32
        dma = pltpu.SemaphoreType.DMA
        result = pl.pallas_call(
            functools.partial(kernel, sections, row_count, col_count),
            out_shape=jax.ShapeDtypeStruct((groups, rows, pieces), f32),
            in_specs=[
                pl.BlockSpec(memory_space=pltpu.VMEM),
                pl.BlockSpec(memory_space=pltpu.HBM),
                pl.BlockSpec(memory_space=pltpu.VMEM),
            ],
            out_specs=pl.BlockSpec(memory_space=pltpu.VMEM),
            scratch_shapes=[
                pltpu.VMEM((groups, row_count, rows, pieces), f32),
                pltpu.VMEM((groups, row_count, rows, pieces), f32),
                pltpu.VMEM((2 * rows, depth), jnp.bfloat16),
                pltpu.VMEM((groups, col_count, rows, pieces), f32),
                pltpu.VMEM((groups, col_count + 1, rows, pieces), f32),
                pltpu.VMEM((groups, rows, pieces), f32),
                pltpu.VMEM((128, 128), f32),
                pltpu.VMEM((groups, rows, 128), f32),
                pltpu.VMEM((groups, rows, 128), f32),
                pltpu.VMEM((RING + kept, depth, width), f32),
                pltpu.VMEM((groups, 8, 128), f32),
                pltpu.VMEM((groups, col_count, 8, 128), f32),
                pltpu.VMEM((groups, 8, 128), f32),
                pltpu.VMEM((groups, row_count, 8, 128), f32),
                dma((RING + kept,)),
                dma((groups, row_count)),
                dma((groups, row_count)),
                dma((groups, row_count)),
                dma((groups, row_count)),
                dma((groups, col_count)),
                dma((groups, col_count + 1)),
                dma((groups, col_count)),
                dma((groups, col_count)),
                dma((groups, row_count)),
                dma((groups, row_count)),
                dma((groups,)),
                dma((groups,)),
                dma((groups,)),
                dma((groups,)),
            ],
            compiler_params=pltpu.CompilerParams(
                collective_id=0, has_side_effects=True, vmem_limit_bytes=67043328
            ),
        )(inputs.reshape(groups, rows, pieces), weights.reshape(depth, out_cols), norm_gain)
        return result.reshape(1, micro, batch, pieces)

    placed = (
        P(None, None, ("row", "col")),
        P("section", None, "col", None, "row"),
        P("section", ("row", "col")),
    )
    return jax.shard_map(
        shards,
        mesh=mesh,
        in_specs=placed,
        out_specs=P("section", None, None, ("row", "col")),
        check_vma=False,
    )
```

```python
import functools

import jax
import jax.numpy as jnp
from jax import lax
from jax.experimental import pallas as pl
from jax.experimental.pallas import tpu as pltpu
from jax.sharding import PartitionSpec as P

MESH = pl.DeviceIdType.MESH
SPAN = 16
RING = 3
KEEP = 4
PARTS = 2
LAG = 2
ACT = 2
PASS = 3
NORM = 2
LATE = 2


def slices(values):
    first = values.astype(jnp.bfloat16)
    second = (values - first.astype(jnp.float32)).astype(jnp.bfloat16)
    return first, second


def sending_order(col_count):
    table = []
    for here in range(col_count):
        keys = []
        for there in range(col_count):
            if there > here:
                keys.append((col_count - 1 - there + here, there))
            elif there < here:
                keys.append((there + col_count - 1 - here, there))
        table.append([there for _, there in sorted(keys)] + [here])
    return table


def kernel(
    sections, row_count, col_count,
    x_ref, w_ref, gain_ref, out_ref,
    gathered, branch, lhs, part, landed, scaled, squares, factor, factor_in, tiles,
    col_out, col_in, row_out, row_in,
    tile_sem, gx_send, gx_recv, gy_send, gy_recv, rs_send, rs_recv,
    col_send, col_recv, row_send, row_recv, next_send, next_recv, fac_send, fac_recv,
):
    groups, rows, pieces = x_ref.shape
    width = tiles.shape[2]
    per_chunk = pieces // width
    steps = per_chunk * col_count
    kept = steps // KEEP
    total_features = pieces * row_count * col_count
    section = lax.axis_index("section")
    row = lax.axis_index("row")
    col = lax.axis_index("col")
    cores = 2 if row_count % 2 == 0 else 1
    chips = row_count // cores
    core = lax.rem(row, cores)
    chip = row // cores
    edge = (col == 0) | (col == col_count - 1)
    inner = (col > 0) & (col < col_count - 1)
    first_section = section == 0
    table = sending_order(col_count)

    places = []
    for place in range(col_count):
        found = jnp.int32(table[0][place])
        for here in range(1, col_count):
            found = jnp.where(col == here, table[here][place], found)
        places.append(found)

    def passing(k):
        found = places[0]
        for place in range(1, col_count):
            found = jnp.where(k == place, places[place], found)
        return found

    def around(position, step, count):
        return lax.rem(position + step, count)

    def chip_row(step, which):
        return around(chip, step, chips) * cores + which

    def remote(src, dst, send, recv, device):
        return pltpu.make_async_remote_copy(
            src_ref=src, dst_ref=dst, send_sem=send, recv_sem=recv,
            device_id=device, device_id_type=MESH,
        )

    def slot_of(m, q):
        stream = m * (steps - kept) + q - q // KEEP - 1
        return jnp.where(lax.rem(q, KEEP) == 0, RING + q // KEEP, lax.rem(jnp.maximum(stream, 0), RING))

    def fetch(m, q):
        start = passing(q // per_chunk) * pieces + lax.rem(q, per_chunk) * width
        slot = slot_of(m, q)
        return pltpu.make_async_copy(
            w_ref.at[:, pl.ds(pl.multiple_of(start, width), width)],
            tiles.at[slot], tile_sem.at[slot],
        )

    def fetched(m, q):
        return (m == 0) | (lax.rem(q, KEEP) != 0)

    for q in range(RING):
        fetch(0, q).start()

    barrier = pltpu.get_barrier_semaphore()
    for step in range(1, row_count):
        pl.semaphore_signal(barrier, inc=1, device_id={"row": around(row, step, row_count)}, device_id_type=MESH)
    for step in range(1, col_count):
        pl.semaphore_signal(barrier, inc=1, device_id={"col": around(col, step, col_count)}, device_id_type=MESH)

    @pl.when(section > 0)
    def _():
        pl.semaphore_signal(barrier, inc=1, device_id={"section": section - 1}, device_id_type=MESH)

    @pl.when(section < sections - 1)
    def _():
        pl.semaphore_signal(barrier, inc=1, device_id={"section": section + 1}, device_id_type=MESH)

    before = (section + sections - 1) // sections
    after = (2 * (sections - 1) - section) // sections
    pl.semaphore_wait(barrier, row_count + col_count - 2 + before + after)

    def gather_send(buffer, send, recv, m, target):
        return remote(buffer.at[m, row], buffer.at[m, row], send.at[m, target], recv.at[m, row], {"row": target})

    def gather_start(buffer, send, recv, m):
        for step in range(1, chips):
            gather_send(buffer, send, recv, m, chip_row(step, core)).start()
        if cores == 2:
            gather_send(buffer, send, recv, m, chip * cores + 1 - core).start()

    def gather_forward(buffer, send, recv, m, step):
        held = chip_row(step, core)
        slot = chip_row(step, 1 - core)
        return remote(
            buffer.at[m, held], buffer.at[m, held], send.at[m, slot],
            recv.at[m, held], {"row": chip * cores + 1 - core},
        )

    def gather_landed(buffer, send, recv, m, source):
        target = around(row, 1, row_count)
        remote(buffer.at[m, source], buffer.at[m, source], send.at[m, source],
               recv.at[m, source], {"row": target}).wait_recv()

    def gather_relay(buffer, send, recv, m):
        for step in range(1, chips):
            gather_landed(buffer, send, recv, m, chip_row(step, core))
            if cores == 2:
                gather_forward(buffer, send, recv, m, step).start()

    def gather_rest(buffer, send, recv, m):
        if cores == 2:
            for step in range(chips):
                gather_landed(buffer, send, recv, m, chip_row(step, 1 - core))

    def gather_drain(buffer, send, recv, m):
        for step in range(1, chips):
            gather_send(buffer, send, recv, m, chip_row(step, core)).wait_send()
            if cores == 2:
                gather_forward(buffer, send, recv, m, step).wait_send()
        if cores == 2:
            gather_send(buffer, send, recv, m, chip * cores + 1 - core).wait_send()

    gx = (gathered, gx_send, gx_recv)
    gy = (branch, gy_send, gy_recv)

    def x_start(m):
        gathered[m, row] = x_ref[m]
        gather_start(*gx, m)

    def hand(m, target):
        return remote(scaled.at[m], branch.at[m, row], next_send.at[m], next_recv.at[m], {"section": target})

    def hand_factor(m, target):
        return remote(factor.at[m], factor_in.at[m], fac_send.at[m], fac_recv.at[m], {"section": target})

    def unit(m, there):
        upward = (there > col).astype(jnp.int32)
        slot = there + upward
        return remote(part.at[m, there], landed.at[m, slot], rs_send.at[m, there],
                      rs_recv.at[m, slot], {"col": col + 2 * upward - 1})

    def take(m, slot, there):
        remote(part.at[m, there], landed.at[m, slot], rs_send.at[m, there],
               rs_recv.at[m, slot], {"col": around(col, 1, col_count)}).wait_recv()

        def grow(g, carry):
            span = pl.ds(pl.multiple_of(g * SPAN, SPAN), SPAN)
            part[m, there, span, :] += landed[m, slot, span, :]
            return carry
        lax.fori_loop(0, rows // SPAN, grow, 0)

    def forward(m, k):
        there = passing(k)
        take(m, there + (there > col).astype(jnp.int32), there)
        unit(m, there).start()

    def issue(m, i):
        @pl.when(i >= LAG)
        def _():
            unit(m, passing(i - LAG)).wait_send()

        @pl.when((i < LAG) & (m > 0))
        def _():
            unit(m - 1, passing(col_count - 1 + i - LAG)).wait_send()
        unit(m, passing(i)).start()

    def share_start(m, outgoing, incoming, send, recv, axis, position, count):
        for step in range(1, count):
            target = around(position, step, count)
            remote(outgoing.at[m], incoming.at[m, position], send.at[m, target],
                   recv.at[m, position], {axis: target}).start()

    def share_total(m, outgoing, incoming, send, recv, axis, position, count):
        total = outgoing[m]
        for step in range(1, count):
            source = around(position, step, count)
            remote(outgoing.at[m], incoming.at[m, source], send.at[m, source],
                   recv.at[m, source], {axis: source}).wait_recv()
            total = total + incoming[m, source]
        for step in range(1, count):
            target = around(position, step, count)
            remote(outgoing.at[m], incoming.at[m, position], send.at[m, target],
                   recv.at[m, position], {axis: target}).wait_send()
        return total

    by_row = (row_out, row_in, row_send, row_recv, "row", row, row_count)
    by_col = (col_out, col_in, col_send, col_recv, "col", col, col_count)

    def activate(m):
        @pl.when(col > 0)
        def _():
            take(m, col + 1, col)

        @pl.when(col < col_count - 1)
        def _():
            take(m, col, col)

        def spans(g, carry):
            span = pl.ds(pl.multiple_of(g * SPAN, SPAN), SPAN)
            y = jax.nn.gelu(part[m, col, span, :], approximate=True)
            scaled[m, span, :] = y * gain_ref[...]
            squares[span, :] = jnp.broadcast_to(jnp.sum(y * y, axis=1, keepdims=True), (SPAN, 128))
            return carry
        lax.fori_loop(0, rows // SPAN, spans, 0)

        @pl.when(section < sections - 1)
        def _():
            hand(m, section + 1).start()
        row_out[m] = squares[...].T[:8]
        share_start(m, *by_row)

    def pass_on(m):
        col_out[m] = share_total(m, *by_row)
        share_start(m, *by_col)

    def normalize(m):
        total = share_total(m, *by_col)
        scale = lax.rsqrt(total[:1] / total_features + 1e-06)
        squares[...] = jnp.broadcast_to(scale, (128, 128)).T
        factor[m] = squares[:rows]

        @pl.when(section < sections - 1)
        def _():
            hand_factor(m, section + 1).start()

        def spans(g, carry):
            span = pl.ds(pl.multiple_of(g * SPAN, SPAN), SPAN)
            out_ref[m, span, :] = scaled[m, span, :] * factor[m, span, :1]
            return carry
        lax.fori_loop(0, rows // SPAN, spans, 0)

    def prepare(m, added):
        def body(r, carry):
            lanes = pl.ds(pl.multiple_of(r * pieces, pieces), pieces)
            for start in range(0, rows, SPAN):
                values = gathered[m, r, start:start + SPAN]
                if added:
                    values = values + branch[m, r, start:start + SPAN] * factor_in[m, start:start + SPAN, :1]
                first, second = slices(values)
                lhs[start:start + SPAN, lanes] = first
                lhs[rows + start:rows + start + SPAN, lanes] = second
            return carry
        lax.fori_loop(0, row_count, body, 0)

    def acquire(m):
        @pl.when(first_section)
        def _():
            @pl.when(m == 0)
            def _():
                gather_relay(*gx, m)
            gather_rest(*gx, m)

            @pl.when(m + 1 < groups)
            def _():
                x_start(m + 1)
            prepare(m, False)

        @pl.when(section > 0)
        def _():
            @pl.when(m == 0)
            def _():
                def early(n, carry):
                    gather_relay(*gx, n)
                    gather_rest(*gx, n)
                    return carry
                lax.fori_loop(0, groups, early, 0)
                hand(m, section - 1).wait_recv()
                gather_start(*gy, m)
            gather_relay(*gy, m)
            gather_rest(*gy, m)
            hand_factor(m, section - 1).wait_recv()
            prepare(m, True)

    def multiply(m, i):
        there = passing(i)

        def tile_body(j, carry):
            q = i * per_chunk + j
            ahead = m * steps + q + RING
            ahead_m = ahead // steps
            ahead_q = lax.rem(ahead, steps)

            @pl.when((ahead < groups * steps) & fetched(ahead_m, ahead_q))
            def _():
                fetch(ahead_m, ahead_q).start()

            @pl.when(fetched(m, q))
            def _():
                fetch(m, q).wait()
            first, second = slices(tiles[slot_of(m, q)])
            both = jnp.dot(lhs[...], first, preferred_element_type=jnp.float32)
            low = jnp.dot(lhs[:rows], second, preferred_element_type=jnp.float32)
            part[m, there, :, pl.ds(pl.multiple_of(j * width, width), width)] = both[:rows] + (both[rows:] + low)
            return carry
        lax.fori_loop(0, per_chunk, tile_body, 0)

    @pl.when(first_section)
    def _():
        x_start(0)

    @pl.when(section > 0)
    def _():
        def begin(m, carry):
            x_start(m)
            return carry
        lax.fori_loop(0, groups, begin, 0)

    def group_body(m, carry):
        last = m - 1

        @pl.when(m < groups)
        def _():
            acquire(m)

        def chunk_body(i, carry):
            @pl.when(m < groups)
            def _():
                multiply(m, i)

            @pl.when((i < col_count - 1) & (m < groups) & edge)
            def _():
                issue(m, i)

            @pl.when((i == 0) & (m > 0) & inner)
            def _():
                def rest(k, carry):
                    forward(last, k)
                    return carry
                lax.fori_loop(2, col_count - 1, rest, 0)

            @pl.when((i >= col_count - 2) & (m < groups) & inner)
            def _():
                forward(m, i - (col_count - 2))

            soon = (m == 1) | (m == groups)

            @pl.when((i == LATE) & (m > 2))
            def _():
                normalize(m - 2)

            @pl.when((i == jnp.where(soon, 0, ACT)) & (m > 0))
            def _():
                activate(last)

            @pl.when((i == jnp.where(soon, 0, PASS)) & (m > 0))
            def _():
                pass_on(last)

            @pl.when((i == NORM) & soon)
            def _():
                normalize(last)

            @pl.when((i == col_count - 2) & (m + 1 < groups))
            def _():
                @pl.when(first_section)
                def _():
                    gather_relay(*gx, m + 1)

                @pl.when(section > 0)
                def _():
                    hand(m + 1, section - 1).wait_recv()
                    gather_start(*gy, m + 1)
            return carry
        lax.fori_loop(0, col_count, chunk_body, 0)
        return carry
    lax.fori_loop(0, groups + 1, group_body, 0)

    @pl.when(edge)
    def _():
        for i in range(LAG):
            unit(groups - 1, passing(col_count - 2 - i)).wait_send()

    def drain(m, carry):
        gather_drain(*gx, m)

        @pl.when(section > 0)
        def _():
            gather_drain(*gy, m)

        @pl.when(section < sections - 1)
        def _():
            hand(m, section + 1).wait_send()
            hand_factor(m, section + 1).wait_send()

        @pl.when(inner)
        def _():
            def sent(k, carry):
                unit(m, passing(k)).wait_send()
                return carry
            lax.fori_loop(0, col_count - 1, sent, 0)
        return carry
    lax.fori_loop(0, groups, drain, 0)


def solution(mesh):
    sections, row_count, col_count = (mesh.shape[name] for name in ("section", "row", "col"))

    def shards(inputs, weights, norm_gain):
        micro, batch, pieces = inputs.shape
        groups, rows = micro * PARTS, batch // PARTS
        depth = row_count * pieces
        out_cols = weights.shape[4]
        width = min(256, pieces)
        kept = (out_cols // width) // KEEP
        f32 = jnp.float32
        dma = pltpu.SemaphoreType.DMA
        result = pl.pallas_call(
            functools.partial(kernel, sections, row_count, col_count),
            out_shape=jax.ShapeDtypeStruct((groups, rows, pieces), f32),
            in_specs=[
                pl.BlockSpec(memory_space=pltpu.VMEM),
                pl.BlockSpec(memory_space=pltpu.HBM),
                pl.BlockSpec(memory_space=pltpu.VMEM),
            ],
            out_specs=pl.BlockSpec(memory_space=pltpu.VMEM),
            scratch_shapes=[
                pltpu.VMEM((groups, row_count, rows, pieces), f32),
                pltpu.VMEM((groups, row_count, rows, pieces), f32),
                pltpu.VMEM((2 * rows, depth), jnp.bfloat16),
                pltpu.VMEM((groups, col_count, rows, pieces), f32),
                pltpu.VMEM((groups, col_count + 1, rows, pieces), f32),
                pltpu.VMEM((groups, rows, pieces), f32),
                pltpu.VMEM((128, 128), f32),
                pltpu.VMEM((groups, rows, 128), f32),
                pltpu.VMEM((groups, rows, 128), f32),
                pltpu.VMEM((RING + kept, depth, width), f32),
                pltpu.VMEM((groups, 8, 128), f32),
                pltpu.VMEM((groups, col_count, 8, 128), f32),
                pltpu.VMEM((groups, 8, 128), f32),
                pltpu.VMEM((groups, row_count, 8, 128), f32),
                dma((RING + kept,)),
                dma((groups, row_count)),
                dma((groups, row_count)),
                dma((groups, row_count)),
                dma((groups, row_count)),
                dma((groups, col_count)),
                dma((groups, col_count + 1)),
                dma((groups, col_count)),
                dma((groups, col_count)),
                dma((groups, row_count)),
                dma((groups, row_count)),
                dma((groups,)),
                dma((groups,)),
                dma((groups,)),
                dma((groups,)),
            ],
            compiler_params=pltpu.CompilerParams(
                collective_id=0, has_side_effects=True, vmem_limit_bytes=67043328
            ),
        )(inputs.reshape(groups, rows, pieces), weights.reshape(depth, out_cols), norm_gain)
        return result.reshape(1, micro, batch, pieces)

    placed = (
        P(None, None, ("row", "col")),
        P("section", None, "col", None, "row"),
        P("section", ("row", "col")),
    )
    return jax.shard_map(
        shards,
        mesh=mesh,
        in_specs=placed,
        out_specs=P("section", None, None, ("row", "col")),
        check_vma=False,
    )
```
